32 devices in a mesh: dp: 8 (over z, x), tensor: 4 (over y, core).
Axes of the slice: x: 2, y: 2, z: 4, core: 2. Of those that a mesh axis runs over, the one named last changes fastest.
Arguments:
- tokens: bfloat16 [8, 256, 4096], P('dp', 'tensor'), may hold values from -6 to 6
- gain: bfloat16 [4096], replicated, may hold values from 0.5 to 1.5
- wq: bfloat16 [4096, 4096], P(None, 'tensor'), may hold values from -0.09375 to 0.09375
- bq: bfloat16 [4096], P('tensor'), may hold values from -5 to 5
- wkv: bfloat16 [4096, 1024], P(None, 'tensor'), may hold values from -0.09375 to 0.09375
- bkv: bfloat16 [1024], P('tensor'), may hold values from -5 to 5
- wo: bfloat16 [4096, 4096], P('tensor'), may hold values from -0.375 to 0.375
- check_weights: float32 [8, 256], P('dp'), may hold values from -12 to 12
Outputs:
- attended: bfloat16 [8, 256, 4096], P('dp', 'tensor')
- checksum: float32 [4096], replicated
The draws below stay inside these ranges and needn't reach their ends.
All inputs are finite; a program needn't handle non-finite values.
Results may differ from the reference program's by a relative error of at most 0.018.
Values may be sent and summed in bfloat16 or wider, within the bound.
A program may use at most 64 MiB of HBM per device.

```python
import jax
import jax.numpy as jnp
from jax import lax

D = 4096
HEADS = 32
KV = 4
HD = 128
SEQ = 256
GROUPS = 8
N_TENSOR = 4


def draw_check_weights(key, part):
    rising = jnp.exp(jnp.log(3.0) * jnp.arange(GROUPS, dtype=jnp.float32) / max(GROUPS - 1, 1))
    base = jax.random.truncated_normal(key, -4.0, 4.0, (GROUPS, SEQ), jnp.float32)
    return (base * rising[:, None]).astype(jnp.float32)


def draw_bq(key, part):
    return (0.5 * jax.random.truncated_normal(jax.random.fold_in(key, 12), -6.0, 6.0, (HEADS * HD,), jnp.float32)).astype(jnp.bfloat16)


def draw_bkv(key, part):
    value_part = 0.5 * jax.random.truncated_normal(jax.random.fold_in(key, 13), -6.0, 6.0, (KV * HD,), jnp.float32)
    key_part = 0.5 * jax.random.truncated_normal(jax.random.fold_in(key, 15), -6.0, 6.0, (KV * HD,), jnp.float32)
    return jnp.concatenate([key_part, value_part], axis=0).astype(jnp.bfloat16)


def steps_of(own_key, dims, cuts, low, largest):
    loudness, own = 1.0, jax.random.fold_in(own_key, 6)
    for dim, parts in cuts:
        steps = jnp.exp(jax.random.uniform(jax.random.fold_in(own, dim), (parts,), jnp.float32, low / len(cuts), largest / len(cuts)))
        loudness = loudness * jnp.repeat(steps, dims[dim] // parts).reshape([-1 if axis == dim else 1 for axis in range(len(dims))])
    return loudness


def noise(stream_key, dims, width, bound, cuts=(), kind=jnp.bfloat16):
    level = steps_of(stream_key, dims, cuts, -0.22, 0.18) if cuts else 1.0
    entries = jax.random.normal(stream_key, dims, jnp.float32) * width * level
    return jnp.minimum(jnp.maximum(entries, -bound), bound).astype(kind)


def setup_inputs(seed: int = 0) -> dict:
    arg_keys = jax.random.split(jax.random.key(seed), 9)
    tokens = noise(arg_keys[0], (GROUPS, SEQ, D), 1.0, 6.0, ((0, 8), (1, 4)))
    gain = jnp.clip(1.0 + 0.1 * jax.random.normal(arg_keys[1], (D,), jnp.float32), 0.5, 1.5).astype(jnp.bfloat16)
    wq = noise(arg_keys[2], (D, HEADS * HD), D ** -0.5, 0.09375, ((1, 4),))
    bq = draw_bq(jax.random.fold_in(arg_keys[8], 71), 0)
    wkv = noise(arg_keys[4], (D, 2 * KV * HD), D ** -0.5, 0.09375, ((1, 4),))
    bkv = draw_bkv(jax.random.fold_in(arg_keys[8], 71), 0)
    wo = noise(arg_keys[6], (HEADS * HD, D), (HEADS * HD // 16) ** -0.5, 0.375, ((0, 4),))
    check_weights = draw_check_weights(jax.random.fold_in(arg_keys[8], 71), 0)
    return {"tokens": tokens, "gain": gain, "wq": wq, "bq": bq, "wkv": wkv, "bkv": bkv, "wo": wo, "check_weights": check_weights}


EPS = 1e-06
THETA = 1000000.0

def rope(values, head_size):
    rows = values.shape[0]
    half = head_size // 2
    inverse = THETA ** (-(jnp.arange(half, dtype=jnp.float32) * 2.0 / head_size))
    angles = jnp.arange(rows, dtype=jnp.float32)[:, None] * inverse[None, :]
    cosine = jnp.cos(angles)[:, None, :]
    sine = jnp.sin(angles)[:, None, :]
    shaped = values.reshape(rows, -1, head_size)
    first = shaped[..., :half]
    second = shaped[..., half:]
    turned = jnp.concatenate([first * cosine - second * sine, second * cosine + first * sine], axis=-1)
    return turned.reshape(rows, -1)

def reference(tokens, gain, wq, bq, wkv, bkv, wo, check_weights):
    per_dev = HEADS // N_TENSOR * HD
    ratio = HEADS // KV
    scale = HD ** (-0.5)
    causal = jnp.arange(SEQ)[:, None] >= jnp.arange(SEQ)[None, :]

    def one_group(inputs):
        tokens_g, weights_g = inputs
        states = tokens_g.astype(jnp.float32)
        normed = (states * lax.rsqrt(lax.optimization_barrier(jnp.mean(states * states, axis=-1, keepdims=True)) + EPS) * gain.astype(jnp.float32)).astype(jnp.bfloat16)
        query = rope(jnp.dot(normed, wq, preferred_element_type=jnp.float32) + bq.astype(jnp.float32), HD).astype(jnp.bfloat16)
        pairs = (jnp.dot(normed, wkv, preferred_element_type=jnp.float32) + bkv.astype(jnp.float32)).astype(jnp.bfloat16)
        keys = rope(pairs[:, :KV * HD].astype(jnp.float32), HD).astype(jnp.bfloat16)
        values = pairs[:, KV * HD:]

        def one_head(index):
            index = index.astype(jnp.int32)
            shared = (index // ratio).astype(jnp.int32)
            q_head = lax.dynamic_slice_in_dim(query, index * HD, HD, 1).astype(jnp.float32)
            k_head = lax.dynamic_slice_in_dim(keys, shared * HD, HD, 1).astype(jnp.float32)
            v_head = lax.dynamic_slice_in_dim(values, shared * HD, HD, 1).astype(jnp.float32)
            scores = jnp.dot(q_head, k_head.T, precision=lax.Precision.HIGHEST) * scale
            scores = jnp.where(causal, scores, -1e+30)
            probs = jax.nn.softmax(scores, axis=-1).astype(jnp.bfloat16)
            return jnp.dot(probs.astype(jnp.float32), v_head, precision=lax.Precision.HIGHEST).astype(jnp.bfloat16)
        heads_out = lax.map(one_head, jnp.arange(HEADS, dtype=jnp.int32))
        context = jnp.transpose(heads_out, (1, 0, 2)).reshape(SEQ, HEADS * HD)

        def add_part(total, index):
            index = index.astype(jnp.int32)
            piece = lax.dynamic_slice_in_dim(context, index * per_dev, per_dev, 1)
            rows = lax.dynamic_slice_in_dim(wo, index * per_dev, per_dev, 0)
            rounded = jnp.dot(piece, rows, preferred_element_type=jnp.float32).astype(jnp.bfloat16)
            rounded = lax.optimization_barrier(rounded)
            return (total + rounded.astype(jnp.float32), None)
        total, _ = lax.scan(add_part, jnp.zeros((SEQ, D), jnp.float32), jnp.arange(N_TENSOR, dtype=jnp.int32))
        summary = jnp.dot(weights_g, context.astype(jnp.float32), precision=lax.Precision.HIGHEST)
        term = jnp.dot(summary, wo.astype(jnp.float32), precision=lax.Precision.HIGHEST)
        return (total.astype(jnp.bfloat16), term)
    attended, terms = lax.map(one_group, (tokens, check_weights))
    checksum = lax.optimization_barrier(jnp.sum(terms, axis=0)) / jnp.sqrt(jnp.float32(SEQ * GROUPS))
    return (attended, checksum)
```

```python
import functools

import jax
import jax.numpy as jnp
import numpy as np
from jax import lax
from jax.experimental import pallas as pl
from jax.experimental.pallas import tpu as pltpu
from jax.sharding import PartitionSpec as P

HEADS = 32
KV = 4
HD = 128


EPS = 1e-06
THETA = 1000000.0
MESH = pl.DeviceIdType.MESH
F32 = jnp.float32
BF16 = jnp.bfloat16


def rope(values, head_size):
    rows = values.shape[0]
    half = head_size // 2
    inverse = THETA ** (-(jnp.arange(half, dtype=jnp.float32) * 2.0 / head_size))
    angles = jnp.arange(rows, dtype=jnp.float32)[:, None] * inverse[None, :]
    cosine = jnp.cos(angles)[:, None, :]
    sine = jnp.sin(angles)[:, None, :]
    shaped = values.reshape(rows, -1, head_size)
    first = shaped[..., :half]
    second = shaped[..., half:]
    turned = jnp.concatenate(
        [first * cosine - second * sine, second * cosine + first * sine], axis=-1
    )
    return turned.reshape(rows, -1)


def general(tokens, gain, wq, bq, wkv, bkv, wo, check_weights):
    states = tokens[0].astype(jnp.float32)
    normed = (
        states
        * lax.rsqrt(jnp.mean(states * states, axis=-1, keepdims=True) + EPS)
        * gain.astype(jnp.float32)
    ).astype(jnp.bfloat16)
    position = lax.axis_index("tensor")
    head_dev = wq.shape[1] // HD
    query_cols = head_dev * HD
    shared = position * head_dev // (HEADS // KV)
    joined_w = jnp.concatenate([wq, wkv], axis=1)
    joined_b = jnp.concatenate([bq, bkv], axis=0).astype(jnp.float32)
    projected = (
        jnp.dot(
            lax.all_gather(normed, "tensor", axis=0, tiled=True),
            joined_w,
            preferred_element_type=jnp.float32,
        )
        + joined_b[None, :]
    )
    seq_rows = projected.shape[0]
    query = rope(projected[:, :query_cols], HD).astype(jnp.bfloat16)
    kv_local = projected[:, query_cols:].astype(jnp.bfloat16)
    kv_whole = lax.all_gather(kv_local, "tensor", axis=1, tiled=True)
    key_part = lax.dynamic_slice_in_dim(kv_whole, shared * HD, HD, 1)
    values = lax.dynamic_slice_in_dim(kv_whole, KV * HD + shared * HD, HD, 1)
    keys = rope(key_part.astype(jnp.float32), HD).astype(jnp.bfloat16)
    scale = HD ** (-0.5)
    block = min(512, seq_rows)
    query_heads = query.reshape(seq_rows, head_dev, HD)
    pieces = []
    for number in range(seq_rows // block):
        stop = (number + 1) * block
        query_block = query_heads[number * block : stop]
        scores = (
            jnp.einsum("qhd,kd->hqk", query_block, keys[:stop], preferred_element_type=jnp.float32)
            * scale
        )
        allowed = jnp.arange(block)[:, None] + number * block >= jnp.arange(stop)[None, :]
        scores = jnp.where(allowed[None, :, :], scores, -1e30)
        probs = jax.nn.softmax(scores, axis=-1).astype(jnp.bfloat16)
        mixed = jnp.einsum(
            "hqk,kd->qhd", probs, values[:stop], preferred_element_type=jnp.float32
        ).astype(jnp.bfloat16)
        pieces.append(mixed.reshape(block, query_cols))
    context = jnp.concatenate(pieces, axis=0)
    summed = lax.psum_scatter(
        jnp.dot(context, wo, preferred_element_type=jnp.float32).astype(jnp.bfloat16),
        "tensor",
        scatter_dimension=0,
        tiled=True,
    )
    attended = summed[None, :, :]
    summary = jnp.dot(
        check_weights[0], context.astype(jnp.float32), precision=lax.Precision.HIGHEST
    )
    summary = lax.psum(summary, "dp")
    term = jnp.dot(summary, wo.astype(jnp.float32), precision=lax.Precision.HIGHEST)
    total = lax.psum(term, "tensor")
    checksum = total / jnp.sqrt(jnp.float32(seq_rows * lax.axis_size("dp")))
    return (attended, checksum)


def split3(row, count=16):
    high = row.astype(BF16).astype(F32)
    rest = row - high
    middle = rest.astype(BF16).astype(F32)
    low = rest - middle
    index = lax.broadcasted_iota(jnp.int32, (count, row.shape[1]), 0)
    wide = (count, row.shape[1])
    rows = jnp.where(
        index == 0,
        jnp.broadcast_to(high, wide),
        jnp.where(
            index == 1,
            jnp.broadcast_to(middle, wide),
            jnp.where(index == 2, jnp.broadcast_to(low, wide), 0.0),
        ),
    )
    return rows.astype(BF16)


def fused_kernel(
    ndp, kc, nc,
    tok, gain, wq, bq, wkv, bkv, wo, cw, cos, sin,
    out, chk,
    xs, ws, wos, acc, coss, sins, kvl, kvd, keys, ctx, ctxp,
    p_s, p_r, f_s, f_r, q_s, q_r, keep, mine, sum_s, sum_r, term_s, term_r,
    w_sem, wo_sem, t_sem, far_s, far_r, near_s, near_r, fwd_s, fwd_r, kv_s, kv_r,
    ps_s, ps_r, fs_s, fs_r, qs_s, qs_r, sm_s, sm_r, tm_s, tm_r,
):
    rows, d = tok.shape
    pair = 2 * rows
    seq = 2 * pair
    qcols = wq.shape[1]
    heads = qcols // HD
    kch = d // kc
    nch = d // nc
    me = lax.axis_index("tensor")
    dp = lax.axis_index("dp")
    chip = me // 2
    core = me % 2
    partner = chip * 2 + (1 - core)
    across = (1 - chip) * 2 + core
    diagonal = (1 - chip) * 2 + (1 - core)

    def rows_of(device):
        return pl.ds(pl.multiple_of(device * rows, rows), rows)

    own_rows = pl.ds(pl.multiple_of(chip * pair, pair), pair)
    other_rows = pl.ds(pl.multiple_of((1 - chip) * pair, pair), pair)

    barrier = pltpu.get_barrier_semaphore()
    for peer in (partner, across, diagonal):
        pl.semaphore_signal(barrier, inc=1, device_id={"tensor": peer}, device_id_type=MESH)
    for step in range(1, ndp):
        pl.semaphore_signal(
            barrier, inc=1, device_id={"dp": (dp + step) % ndp}, device_id_type=MESH
        )

    def load_q(k):
        at = pl.ds(k * kch, kch)
        return pltpu.make_async_copy(wq.at[at, :], ws.at[k, :, pl.ds(0, qcols)], w_sem.at[0, k])

    def load_kv(k):
        at = pl.ds(k * kch, kch)
        return pltpu.make_async_copy(
            wkv.at[at, :], ws.at[k, :, pl.ds(qcols, wkv.shape[1])], w_sem.at[1, k]
        )

    def load_o(n):
        at = pl.ds(n * nch, nch)
        return pltpu.make_async_copy(wo.at[:, at], wos.at[n], wo_sem.at[n])

    for k in range(kc):
        load_q(k).start()
        load_kv(k).start()
    load_cos = pltpu.make_async_copy(cos, coss, t_sem.at[0])
    load_sin = pltpu.make_async_copy(sin, sins, t_sem.at[1])
    load_cos.start()
    load_sin.start()
    for n in range(nc):
        load_o(n).start()

    square = jnp.zeros((rows, kch), F32)
    for k in range(kc):
        part = tok[:, k * kch : (k + 1) * kch].astype(F32)
        square = square + part * part
    inverse = lax.rsqrt(jnp.sum(square, axis=-1, keepdims=True) / d + EPS)
    for k in range(kc):
        part = tok[:, k * kch : (k + 1) * kch].astype(F32)
        scaled = part * inverse * gain[:, k * kch : (k + 1) * kch].astype(F32)
        xs[k, rows_of(me), :] = scaled.astype(BF16)

    pl.semaphore_wait(barrier, 3 + ndp - 1)

    def remote(src, dst, send, recv, peer):
        return pltpu.make_async_remote_copy(
            src_ref=src, dst_ref=dst, send_sem=send, recv_sem=recv,
            device_id={"tensor": peer}, device_id_type=MESH,
        )

    def far(k, block):
        at = xs.at[k, rows_of(block), :]
        return remote(at, at, far_s.at[k], far_r.at[k], across)

    def near(k, block):
        at = xs.at[k, rows_of(block), :]
        return remote(at, at, near_s.at[k], near_r.at[k], partner)

    def forward(k, block):
        at = xs.at[k, rows_of(block), :]
        return remote(at, at, fwd_s.at[k], fwd_r.at[k], partner)

    for k in range(kc):
        near(k, me).start()
        far(k, me).start()

    def project(k, at, first):
        product = jnp.dot(xs[k, at, :], ws[k], preferred_element_type=F32)
        if first:
            acc[at, :] = product
        else:
            acc[at, :] += product

    def own_step(k, first):
        load_q(k).wait()
        load_kv(k).wait()
        near(k, partner).wait_recv()
        project(k, own_rows, first)

    own_step(0, True)

    @pl.loop(1, kc)
    def _(k):
        own_step(k, False)

    kinds = wkv.shape[1] // HD

    def kv_copy(slot, half):
        number = me * kinds + slot
        at = pl.ds(pl.multiple_of(half * pair, pair), pair)
        return remote(
            kvl.at[slot, at, :], kvd.at[number // KV, at, :],
            kv_s.at[slot, half], kv_r.at[number // KV, half], number % KV,
        )

    def kv_wait(kind, half):
        at = pl.ds(pl.multiple_of(half * pair, pair), pair)
        here = kvd.at[kind, at, :]
        return remote(here, here, kv_s.at[0, half], kv_r.at[kind, half], partner)

    def kv_send(half):
        at = pl.ds(pl.multiple_of(half * pair, pair), pair)
        for slot in range(kinds):
            lanes = slice(qcols + slot * HD, qcols + (slot + 1) * HD)
            bias = bkv[:, slot * HD : (slot + 1) * HD].astype(F32)
            kvl[slot, at, :] = (acc[at, lanes] + bias).astype(BF16)
        for slot in range(kinds):
            number = me * kinds + slot

            @pl.when(number % KV != me)
            def _():
                kv_copy(slot, half).start()

            @pl.when(number % KV == me)
            def _():
                kvd[number // KV, at, :] = kvl[slot, at, :]

    kv_send(chip)

    for k in range(kc + 1):
        if k < kc:
            far(k, across).wait_recv()
            forward(k, across).start()
        if k > 0:
            forward(k - 1, diagonal).wait_recv()
            project(k - 1, other_rows, k == 1)
    kv_send(1 - chip)

    load_cos.wait()
    load_sin.wait()
    shared = me * heads // (HEADS // KV)
    for kind in range(2):
        source = (kind * KV + shared) // kinds

        @pl.when(source != me)
        def _():
            for half in range(2):
                kv_wait(kind, half).wait_recv()

    raw = kvd[0, :, :].astype(F32)
    keys[...] = (raw * coss[...] + pltpu.roll(raw, HD // 2, 1) * sins[...]).astype(BF16)

    scale = HD ** (-0.5)
    for h in range(heads):
        lanes = slice(h * HD, (h + 1) * HD)
        for block in range(2):
            at = slice(block * pair, (block + 1) * pair)
            stop = (block + 1) * pair
            query = acc[at, lanes] + bq[:, lanes].astype(F32)
            query = query * coss[at, :] + pltpu.roll(query, HD // 2, 1) * sins[at, :]
            scores = lax.dot_general(
                query.astype(BF16), keys[:stop, :], (((1,), (1,)), ((), ())),
                preferred_element_type=F32,
            ) * scale
            down = lax.broadcasted_iota(jnp.int32, scores.shape, 0) + block * pair
            right = lax.broadcasted_iota(jnp.int32, scores.shape, 1)
            scores = jnp.where(down >= right, scores, -1e30)
            raised = jnp.exp(scores - jnp.max(scores, axis=-1, keepdims=True))
            total = jnp.sum(raised, axis=-1, keepdims=True)
            mixed = jnp.dot(raised.astype(BF16), kvd[1, :stop, :], preferred_element_type=F32)
            mixed = (mixed * (1.0 / total)).astype(BF16)
            ctx[at, lanes] = mixed
            same = 1 - (block - chip) * (block - chip)
            for side in range(2):
                place = 2 * same + 1 - (side - core) * (side - core)
                ctxp[rows_of(place), lanes] = mixed[side * rows : (side + 1) * rows, :]

    def p_copy(n):
        return remote(p_s.at[n], p_r.at[n], ps_s.at[n], ps_r.at[n], partner)

    def f_copy(n):
        return remote(f_s.at[n], f_r.at[n], fs_s.at[n], fs_r.at[n], across)

    def q_copy(n):
        return remote(q_s.at[n], q_r.at[n], qs_s.at[n], qs_r.at[n], partner)

    def cross(n):
        p_copy(n).wait_recv()
        f_s[n] = (keep[n] + p_r[n].astype(F32)).astype(BF16)
        f_copy(n).start()

    def first_part(n):
        load_o(n).wait()
        product = jnp.dot(ctxp[:pair, :], wos[n], preferred_element_type=F32)
        p_s[n] = product[:rows].astype(BF16)
        p_copy(n).start()
        keep[n] = product[rows:]

    first_part(0)

    @pl.loop(1, nc)
    def _(n):
        first_part(n)
        cross(n - 1)

    weighted = jnp.dot(split3(cw[...]), ctx[...], preferred_element_type=F32)
    summary = jnp.sum(weighted, axis=0, keepdims=True)
    sum_s[...] = summary
    sum_r[dp] = summary
    cross(nc - 1)

    def sum_copy(peer, owner):
        return pltpu.make_async_remote_copy(
            src_ref=sum_s, dst_ref=sum_r.at[owner], send_sem=sm_s.at[peer],
            recv_sem=sm_r.at[owner], device_id={"dp": peer}, device_id_type=MESH,
        )

    for step in range(1, ndp):
        sum_copy((dp + step) % ndp, dp).start()

    @pl.loop(0, nc)
    def _(n):
        product = jnp.dot(ctxp[pair:, :], wos[n], preferred_element_type=F32)
        q_s[n] = product[:rows].astype(BF16)
        q_copy(n).start()
        mine[n] = product[rows:]

    for step in range(1, ndp):
        peer = (dp + step) % ndp
        sum_copy(peer, peer).wait_recv()
    whole = sum_r[0]
    for index in range(1, ndp):
        whole = whole + sum_r[index]
    three = split3(whole)
    for n in range(nc):
        lanes = slice(n * nch, (n + 1) * nch)
        product = jnp.dot(three, wos[n], preferred_element_type=F32)
        term = jnp.sum(product, axis=0, keepdims=True)
        term_s[:, lanes] = term
        term_r[me, :, lanes] = term

    def term_copy(peer, owner):
        return remote(term_s, term_r.at[owner], tm_s.at[peer], tm_r.at[owner], peer)

    for peer in (partner, across, diagonal):
        term_copy(peer, me).start()

    for n in range(nc):
        lanes = slice(n * nch, (n + 1) * nch)
        q_copy(n).wait_recv()
        f_copy(n).wait_recv()
        out[:, lanes] = (mine[n] + q_r[n].astype(F32) + f_r[n].astype(F32)).astype(BF16)

    for peer in (partner, across, diagonal):
        term_copy(peer, peer).wait_recv()
    size = np.float32(1.0) / np.sqrt(np.float32(seq * ndp))
    total = term_r[0] + term_r[1] + term_r[2] + term_r[3]
    chk[...] = total * size

    for k in range(kc):
        near(k, me).wait_send()
        far(k, me).wait_send()
        forward(k, across).wait_send()
    for slot in range(kinds):
        for half in range(2):

            @pl.when((me * kinds + slot) % KV != me)
            def _():
                kv_copy(slot, half).wait_send()

    for n in range(nc):
        p_copy(n).wait_send()
        f_copy(n).wait_send()
        q_copy(n).wait_send()
    for step in range(1, ndp):
        sum_copy((dp + step) % ndp, dp).wait_send()
    for peer in (partner, across, diagonal):
        term_copy(peer, me).wait_send()


def tables(seq):
    half = HD // 2
    inverse = THETA ** (-(np.arange(half, dtype=np.float32) * np.float32(2.0) / np.float32(HD)))
    angles = np.arange(seq, dtype=np.float32)[:, None] * inverse[None, :].astype(np.float32)
    cosine = np.cos(angles).astype(np.float32)
    sine = np.sin(angles).astype(np.float32)
    return (
        np.concatenate([cosine, cosine], axis=1),
        np.concatenate([-sine, sine], axis=1),
    )


def fused(ndp, n_tensor, tokens, gain, wq, bq, wkv, bkv, wo, check_weights):
    rows, d = tokens.shape[1:]
    seq = rows * n_tensor
    kc = nc = 8
    kch, nch = d // kc, d // nc
    qcols, kvcols = wq.shape[1], wkv.shape[1]
    cosine, sine = tables(seq)
    vmem = pl.BlockSpec(memory_space=pltpu.VMEM)
    hbm = pl.BlockSpec(memory_space=pl.ANY)
    dma = pltpu.SemaphoreType.DMA
    block = pltpu.VMEM((nc, rows, nch), BF16)
    wide = pltpu.VMEM((nc, rows, nch), F32)
    attended, checksum = pl.pallas_call(
        functools.partial(fused_kernel, ndp, kc, nc),
        out_shape=(
            jax.ShapeDtypeStruct((rows, d), BF16),
            jax.ShapeDtypeStruct((1, d), F32),
        ),
        in_specs=[vmem, vmem, hbm, vmem, hbm, vmem, hbm, vmem, hbm, hbm],
        out_specs=(vmem, vmem),
        scratch_shapes=[
            pltpu.VMEM((kc, seq, kch), BF16),
            pltpu.VMEM((kc, kch, qcols + kvcols), BF16),
            pltpu.VMEM((nc, qcols, nch), BF16),
            pltpu.VMEM((seq, qcols + kvcols), F32),
            pltpu.VMEM((seq, HD), F32),
            pltpu.VMEM((seq, HD), F32),
            pltpu.VMEM((kvcols // HD, seq, HD), BF16),
            pltpu.VMEM((2, seq, HD), BF16),
            pltpu.VMEM((seq, HD), BF16),
            pltpu.VMEM((seq, qcols), BF16),
            pltpu.VMEM((seq, qcols), BF16),
            block, block, block, block, block, block, wide, wide,
            pltpu.VMEM((1, qcols), F32),
            pltpu.VMEM((ndp, 1, qcols), F32),
            pltpu.VMEM((1, d), F32),
            pltpu.VMEM((n_tensor, 1, d), F32),
            dma((2, kc)), dma((nc,)), dma((2,)),
            dma((kc,)), dma((kc,)), dma((kc,)), dma((kc,)), dma((kc,)), dma((kc,)),
            dma((kvcols // HD, 2)), dma((2, 2)),
            dma((nc,)), dma((nc,)), dma((nc,)), dma((nc,)), dma((nc,)), dma((nc,)),
            dma((ndp,)), dma((ndp,)), dma((n_tensor,)), dma((n_tensor,)),
        ],
        compiler_params=pltpu.CompilerParams(
            collective_id=0, has_side_effects=True, vmem_limit_bytes=60 * 1024 * 1024
        ),
    )(
        tokens.reshape(rows, d), gain.reshape(1, d), wq, bq.reshape(1, qcols), wkv,
        bkv.reshape(1, kvcols), wo, check_weights, cosine, sine,
    )
    return attended.reshape(1, rows, d), checksum.reshape(d)


def solution(mesh):
    placed = (
        P("dp", "tensor", None),
        P(),
        P(None, "tensor"),
        P("tensor"),
        P(None, "tensor"),
        P("tensor"),
        P("tensor", None),
        P("dp", None),
    )
    ndp, n_tensor = mesh.shape["dp"], mesh.shape["tensor"]

    def local(tokens, gain, wq, bq, wkv, bkv, wo, check_weights):
        whole_heads = wkv.shape[1] == 2 * HD and wq.shape[1] == HEADS // KV * HD
        if n_tensor == KV and whole_heads:
            return fused(ndp, n_tensor, tokens, gain, wq, bq, wkv, bkv, wo, check_weights)
        return general(tokens, gain, wq, bq, wkv, bkv, wo, check_weights)

    return jax.shard_map(
        local, mesh=mesh, in_specs=placed, out_specs=(P("dp", "tensor", None), P()), check_vma=False
    )
```

```python
import functools

import jax
import jax.numpy as jnp
import numpy as np
from jax import lax
from jax.experimental import pallas as pl
from jax.experimental.pallas import tpu as pltpu
from jax.sharding import PartitionSpec as P

HEADS = 32
KV = 4
HD = 128


EPS = 1e-06
THETA = 1000000.0
MESH = pl.DeviceIdType.MESH
F32 = jnp.float32
BF16 = jnp.bfloat16


def rope(values, head_size):
    rows = values.shape[0]
    half = head_size // 2
    inverse = THETA ** (-(jnp.arange(half, dtype=jnp.float32) * 2.0 / head_size))
    angles = jnp.arange(rows, dtype=jnp.float32)[:, None] * inverse[None, :]
    cosine = jnp.cos(angles)[:, None, :]
    sine = jnp.sin(angles)[:, None, :]
    shaped = values.reshape(rows, -1, head_size)
    first = shaped[..., :half]
    second = shaped[..., half:]
    turned = jnp.concatenate(
        [first * cosine - second * sine, second * cosine + first * sine], axis=-1
    )
    return turned.reshape(rows, -1)


def general(tokens, gain, wq, bq, wkv, bkv, wo, check_weights):
    states = tokens[0].astype(jnp.float32)
    normed = (
        states
        * lax.rsqrt(jnp.mean(states * states, axis=-1, keepdims=True) + EPS)
        * gain.astype(jnp.float32)
    ).astype(jnp.bfloat16)
    position = lax.axis_index("tensor")
    head_dev = wq.shape[1] // HD
    query_cols = head_dev * HD
    shared = position * head_dev // (HEADS // KV)
    joined_w = jnp.concatenate([wq, wkv], axis=1)
    joined_b = jnp.concatenate([bq, bkv], axis=0).astype(jnp.float32)
    projected = (
        jnp.dot(
            lax.all_gather(normed, "tensor", axis=0, tiled=True),
            joined_w,
            preferred_element_type=jnp.float32,
        )
        + joined_b[None, :]
    )
    seq_rows = projected.shape[0]
    query = rope(projected[:, :query_cols], HD).astype(jnp.bfloat16)
    kv_local = projected[:, query_cols:].astype(jnp.bfloat16)
    kv_whole = lax.all_gather(kv_local, "tensor", axis=1, tiled=True)
    key_part = lax.dynamic_slice_in_dim(kv_whole, shared * HD, HD, 1)
    values = lax.dynamic_slice_in_dim(kv_whole, KV * HD + shared * HD, HD, 1)
    keys = rope(key_part.astype(jnp.float32), HD).astype(jnp.bfloat16)
    scale = HD ** (-0.5)
    block = min(512, seq_rows)
    query_heads = query.reshape(seq_rows, head_dev, HD)
    pieces = []
    for number in range(seq_rows // block):
        stop = (number + 1) * block
        query_block = query_heads[number * block : stop]
        scores = (
            jnp.einsum("qhd,kd->hqk", query_block, keys[:stop], preferred_element_type=jnp.float32)
            * scale
        )
        allowed = jnp.arange(block)[:, None] + number * block >= jnp.arange(stop)[None, :]
        scores = jnp.where(allowed[None, :, :], scores, -1e30)
        probs = jax.nn.softmax(scores, axis=-1).astype(jnp.bfloat16)
        mixed = jnp.einsum(
            "hqk,kd->qhd", probs, values[:stop], preferred_element_type=jnp.float32
        ).astype(jnp.bfloat16)
        pieces.append(mixed.reshape(block, query_cols))
    context = jnp.concatenate(pieces, axis=0)
    summed = lax.psum_scatter(
        jnp.dot(context, wo, preferred_element_type=jnp.float32).astype(jnp.bfloat16),
        "tensor",
        scatter_dimension=0,
        tiled=True,
    )
    attended = summed[None, :, :]
    summary = jnp.dot(
        check_weights[0], context.astype(jnp.float32), precision=lax.Precision.HIGHEST
    )
    summary = lax.psum(summary, "dp")
    term = jnp.dot(summary, wo.astype(jnp.float32), precision=lax.Precision.HIGHEST)
    total = lax.psum(term, "tensor")
    checksum = total / jnp.sqrt(jnp.float32(seq_rows * lax.axis_size("dp")))
    return (attended, checksum)


def split3(row, count=16):
    high = row.astype(BF16).astype(F32)
    rest = row - high
    middle = rest.astype(BF16).astype(F32)
    low = rest - middle
    index = lax.broadcasted_iota(jnp.int32, (count, row.shape[1]), 0)
    wide = (count, row.shape[1])
    rows = jnp.where(
        index == 0,
        jnp.broadcast_to(high, wide),
        jnp.where(
            index == 1,
            jnp.broadcast_to(middle, wide),
            jnp.where(index == 2, jnp.broadcast_to(low, wide), 0.0),
        ),
    )
    return rows.astype(BF16)


def fused_kernel(
    ndp, kc, nc,
    tok_h, gain_h, wq, bq_h, wkv, bkv_h, wo, cw_h, cos, sin,
    out, chk,
    tok, gain, bq, bkv, cw, qs, xs, ws, wos, acc, coss, sins, kvl, kvd, keys, ctx, ctxp,
    p_s, p_r, f_s, f_r, q_s, q_r, keep, mine, sum_s, sum_r, term_s, term_r,
    w_sem, wo_sem, t_sem, far_s, far_r, near_s, near_r, fwd_s, fwd_r, kv_s, kv_r,
    ps_s, ps_r, fs_s, fs_r, qs_s, qs_r, sm_s, sm_r, tm_s, tm_r,
):
    rows, d = tok.shape
    pair = 2 * rows
    seq = 2 * pair
    qcols = wq.shape[1]
    heads = qcols // HD
    kch = d // kc
    nch = d // nc
    me = lax.axis_index("tensor")
    dp = lax.axis_index("dp")
    chip = me // 2
    core = me % 2
    partner = chip * 2 + (1 - core)
    across = (1 - chip) * 2 + core
    diagonal = (1 - chip) * 2 + (1 - core)

    def rows_of(device):
        return pl.ds(pl.multiple_of(device * rows, rows), rows)

    own_rows = pl.ds(pl.multiple_of(chip * pair, pair), pair)
    other_rows = pl.ds(pl.multiple_of((1 - chip) * pair, pair), pair)

    barrier = pltpu.get_barrier_semaphore()
    for peer in (partner, across, diagonal):
        pl.semaphore_signal(barrier, inc=1, device_id={"tensor": peer}, device_id_type=MESH)
    bits = ndp.bit_length() - 1

    def twin(bit):
        return dp + 2**bit * (1 - 2 * (dp // 2**bit % 2))

    for bit in range(bits):
        pl.semaphore_signal(barrier, inc=1, device_id={"dp": twin(bit)}, device_id_type=MESH)

    smalls = [
        pltpu.make_async_copy(source, target, t_sem.at[index])
        for index, (source, target) in enumerate(
            ((tok_h, tok), (gain_h, gain), (bq_h, bq), (bkv_h, bkv), (cw_h, cw), (cos, coss), (sin, sins))
        )
    ]
    smalls[0].start()
    smalls[1].start()

    def load_q(k):
        at = pl.ds(k * kch, kch)
        return pltpu.make_async_copy(wq.at[at, :], ws.at[k, :, pl.ds(0, qcols)], w_sem.at[0, k])

    def load_kv(k):
        at = pl.ds(k * kch, kch)
        return pltpu.make_async_copy(
            wkv.at[at, :], ws.at[k, :, pl.ds(qcols, wkv.shape[1])], w_sem.at[1, k]
        )

    def load_o(n):
        at = pl.ds(n * nch, nch)
        return pltpu.make_async_copy(wo.at[:, at], wos.at[n], wo_sem.at[n])

    for k in range(kc):
        load_q(k).start()
        load_kv(k).start()
    for small in smalls[2:]:
        small.start()
    for n in range(nc):
        load_o(n).start()

    smalls[0].wait()
    smalls[1].wait()
    square = jnp.zeros((rows, kch), F32)
    for k in range(kc):
        part = tok[:, k * kch : (k + 1) * kch].astype(F32)
        square = square + part * part
    inverse = lax.rsqrt(jnp.sum(square, axis=-1, keepdims=True) / d + EPS)
    for k in range(kc):
        part = tok[:, k * kch : (k + 1) * kch].astype(F32)
        scaled = part * inverse * gain[k * kch : (k + 1) * kch].astype(F32)[None, :]
        xs[k, rows_of(me), :] = scaled.astype(BF16)

    pl.semaphore_wait(barrier, 3 + bits)

    def remote(src, dst, send, recv, peer):
        return pltpu.make_async_remote_copy(
            src_ref=src, dst_ref=dst, send_sem=send, recv_sem=recv,
            device_id={"tensor": peer}, device_id_type=MESH,
        )

    def far(k, block):
        at = xs.at[k, rows_of(block), :]
        return remote(at, at, far_s.at[k], far_r.at[k], across)

    def near(k, block):
        at = xs.at[k, rows_of(block), :]
        return remote(at, at, near_s.at[k], near_r.at[k], partner)

    def forward(k, block):
        at = xs.at[k, rows_of(block), :]
        return remote(at, at, fwd_s.at[k], fwd_r.at[k], partner)

    for k in range(kc):
        near(k, me).start()
        far(k, me).start()

    def project(k, at, first, begin=0, end=None):
        end = ws.shape[2] if end is None else end
        product = jnp.dot(xs[k, at, :], ws[k, :, begin:end], preferred_element_type=F32)
        if first:
            acc[at, begin:end] = product
        else:
            acc[at, begin:end] += product

    def rope_query(half):
        at = pl.ds(pl.multiple_of(half * pair, pair), pair)
        for h in range(heads):
            lanes = slice(h * HD, (h + 1) * HD)
            query = acc[at, lanes] + bq[lanes].astype(F32)[None, :]
            query = query * coss[at, :] + pltpu.roll(query, HD // 2, 1) * sins[at, :]
            qs[at, lanes] = query.astype(BF16)

    def own_step(k, first):
        load_q(k).wait()
        load_kv(k).wait()
        near(k, partner).wait_recv()
        project(k, own_rows, first)

    own_step(0, True)

    @pl.loop(1, kc)
    def _(k):
        own_step(k, False)

    kinds = wkv.shape[1] // HD

    def kv_copy(slot, half):
        number = me * kinds + slot
        at = pl.ds(pl.multiple_of(half * pair, pair), pair)
        return remote(
            kvl.at[slot, at, :], kvd.at[number // KV, at, :],
            kv_s.at[slot, half], kv_r.at[number // KV, half], number % KV,
        )

    def kv_wait(kind, half):
        at = pl.ds(pl.multiple_of(half * pair, pair), pair)
        here = kvd.at[kind, at, :]
        return remote(here, here, kv_s.at[0, half], kv_r.at[kind, half], partner)

    def kv_send(half):
        at = pl.ds(pl.multiple_of(half * pair, pair), pair)
        for slot in range(kinds):
            lanes = slice(qcols + slot * HD, qcols + (slot + 1) * HD)
            bias = bkv[slot * HD : (slot + 1) * HD].astype(F32)[None, :]
            kvl[slot, at, :] = (acc[at, lanes] + bias).astype(BF16)
        for slot in range(kinds):
            number = me * kinds + slot

            @pl.when(number % KV != me)
            def _():
                kv_copy(slot, half).start()

            @pl.when(number % KV == me)
            def _():
                kvd[number // KV, at, :] = kvl[slot, at, :]

    for small in smalls[2:]:
        small.wait()
    kv_send(chip)

    for k in range(kc + 1):
        if k < kc:
            far(k, across).wait_recv()
            forward(k, across).start()
        if k == 1:
            rope_query(chip)
        if k > 0:
            forward(k - 1, diagonal).wait_recv()
            if k < kc:
                project(k - 1, other_rows, k == 1)
            else:
                project(k - 1, other_rows, k == 1, qcols)
    kv_send(1 - chip)
    project(kc - 1, other_rows, False, 0, qcols)
    rope_query(1 - chip)

    shared = me * heads // (HEADS // KV)
    for kind in range(2):
        source = (kind * KV + shared) // kinds

        @pl.when(source != me)
        def _():
            for half in range(2):
                kv_wait(kind, half).wait_recv()

    raw = kvd[0, :, :].astype(F32)
    keys[...] = (raw * coss[...] + pltpu.roll(raw, HD // 2, 1) * sins[...]).astype(BF16)

    scale = HD ** (-0.5)

    def attend(block):
        at = pl.ds(pl.multiple_of(block * pair, pair), pair)
        same = 1 - (block - chip) * (block - chip)
        for h in range(heads):
            lanes = slice(h * HD, (h + 1) * HD)
            scores = lax.dot_general(
                qs[at, lanes], keys[...], (((1,), (1,)), ((), ())), preferred_element_type=F32
            ) * scale
            down = lax.broadcasted_iota(jnp.int32, scores.shape, 0) + block * pair
            right = lax.broadcasted_iota(jnp.int32, scores.shape, 1)
            scores = jnp.where(down >= right, scores, -1e30)
            raised = jnp.exp(scores - jnp.max(scores, axis=-1, keepdims=True))
            total = jnp.sum(raised, axis=-1, keepdims=True)
            mixed = jnp.dot(raised.astype(BF16), kvd[1, :, :], preferred_element_type=F32)
            mixed = (mixed * (1.0 / total)).astype(BF16)
            ctx[at, lanes] = mixed
            for side in range(2):
                place = 2 * same + 1 - (side - core) * (side - core)
                ctxp[rows_of(place), lanes] = mixed[side * rows : (side + 1) * rows, :]

    attend(1 - chip)

    def p_copy(n):
        return remote(p_s.at[n], p_r.at[n], ps_s.at[n], ps_r.at[n], partner)

    def f_copy(n):
        return remote(f_s.at[n], f_r.at[n], fs_s.at[n], fs_r.at[n], across)

    def q_copy(n):
        return remote(q_s.at[n], q_r.at[n], qs_s.at[n], qs_r.at[n], partner)

    def cross(n):
        p_copy(n).wait_recv()
        f_s[n] = (keep[n] + p_r[n].astype(F32)).astype(BF16)
        f_copy(n).start()

    def first_part(n):
        load_o(n).wait()
        product = jnp.dot(ctxp[:pair, :], wos[n], preferred_element_type=F32)
        p_s[n] = product[:rows].astype(BF16)
        p_copy(n).start()
        keep[n] = product[rows:]

    def sum_copy(bit):
        return pltpu.make_async_remote_copy(
            src_ref=sum_s.at[bit], dst_ref=sum_r.at[bit], send_sem=sm_s.at[bit],
            recv_sem=sm_r.at[bit], device_id={"dp": twin(bit)}, device_id_type=MESH,
        )

    def own_part(n):
        product = jnp.dot(ctxp[pair:, :], wos[n], preferred_element_type=F32)
        q_s[n] = product[:rows].astype(BF16)
        q_copy(n).start()
        mine[n] = product[rows:]

    lead = 3
    first_part(0)
    for n in range(1, lead):
        first_part(n)
        cross(n - 1)
    attend(chip)
    weighted = jnp.dot(split3(cw[...]), ctx[...], preferred_element_type=F32)
    whole = jnp.sum(weighted, axis=0, keepdims=True)
    edges = [lead + (nc - lead) * step // bits for step in range(bits + 1)]
    for bit in range(bits):
        sum_s[bit] = whole
        sum_copy(bit).start()
        for n in range(edges[bit], edges[bit + 1]):
            first_part(n)
            cross(n - 1)
        if bit == bits - 1:
            cross(nc - 1)
        sum_copy(bit).wait_recv()
        whole = whole + sum_r[bit]

    def term_copy(step):
        return remote(
            term_s.at[step], term_r.at[step], tm_s.at[step], tm_r.at[step],
            (partner, across)[step],
        )

    three = split3(whole)
    for n in range(nc):
        lanes = slice(n * nch, (n + 1) * nch)
        product = jnp.dot(three, wos[n], preferred_element_type=F32)
        term_s[0, :, lanes] = jnp.sum(product, axis=0, keepdims=True)
    term_copy(0).start()
    pl.loop(0, nc // 2)(own_part)
    term_copy(0).wait_recv()
    term_s[1] = term_s[0] + term_r[0]
    term_copy(1).start()
    pl.loop(nc // 2, nc)(own_part)

    for n in range(nc):
        lanes = slice(n * nch, (n + 1) * nch)
        q_copy(n).wait_recv()
        f_copy(n).wait_recv()
        out[:, lanes] = (mine[n] + q_r[n].astype(F32) + f_r[n].astype(F32)).astype(BF16)

    term_copy(1).wait_recv()
    size = np.float32(1.0) / np.sqrt(np.float32(seq * ndp))
    chk[...] = (term_s[1] + term_r[1]) * size

    for k in range(kc):
        near(k, me).wait_send()
        far(k, me).wait_send()
        forward(k, across).wait_send()
    for slot in range(kinds):
        for half in range(2):

            @pl.when((me * kinds + slot) % KV != me)
            def _():
                kv_copy(slot, half).wait_send()

    for n in range(nc):
        p_copy(n).wait_send()
        f_copy(n).wait_send()
        q_copy(n).wait_send()
    for bit in range(bits):
        sum_copy(bit).wait_send()
    for step in range(2):
        term_copy(step).wait_send()


def settle_kernel(attended, checksum, out, chk):
    out[...] = attended[...]
    chk[...] = checksum[...].reshape(chk.shape)


def tables(seq):
    half = HD // 2
    inverse = THETA ** (-(np.arange(half, dtype=np.float32) * np.float32(2.0) / np.float32(HD)))
    angles = np.arange(seq, dtype=np.float32)[:, None] * inverse[None, :].astype(np.float32)
    cosine = np.cos(angles).astype(np.float32)
    sine = np.sin(angles).astype(np.float32)
    return (
        np.concatenate([cosine, cosine], axis=1),
        np.concatenate([-sine, sine], axis=1),
    )


def fused(ndp, n_tensor, tokens, gain, wq, bq, wkv, bkv, wo, check_weights):
    rows, d = tokens.shape[1:]
    seq = rows * n_tensor
    kc = nc = 8
    kch, nch = d // kc, d // nc
    qcols, kvcols = wq.shape[1], wkv.shape[1]
    cosine, sine = tables(seq)
    vmem = pl.BlockSpec(memory_space=pltpu.VMEM)
    hbm = pl.BlockSpec(memory_space=pltpu.HBM)
    dma = pltpu.SemaphoreType.DMA
    block = pltpu.VMEM((nc, rows, nch), BF16)
    wide = pltpu.VMEM((nc, rows, nch), F32)
    bits = ndp.bit_length() - 1
    attended, checksum = pl.pallas_call(
        functools.partial(fused_kernel, ndp, kc, nc),
        out_shape=(
            jax.ShapeDtypeStruct((rows, d), BF16),
            jax.ShapeDtypeStruct((1, d), F32),
        ),
        in_specs=[hbm] * 10,
        out_specs=(vmem, vmem),
        scratch_shapes=[
            pltpu.VMEM((rows, d), BF16),
            pltpu.VMEM((d,), BF16),
            pltpu.VMEM((qcols,), BF16),
            pltpu.VMEM((kvcols,), BF16),
            pltpu.VMEM((1, seq), F32),
            pltpu.VMEM((seq, qcols), BF16),
            pltpu.VMEM((kc, seq, kch), BF16),
            pltpu.VMEM((kc, kch, qcols + kvcols), BF16),
            pltpu.VMEM((nc, qcols, nch), BF16),
            pltpu.VMEM((seq, qcols + kvcols), F32),
            pltpu.VMEM((seq, HD), F32),
            pltpu.VMEM((seq, HD), F32),
            pltpu.VMEM((kvcols // HD, seq, HD), BF16),
            pltpu.VMEM((2, seq, HD), BF16),
            pltpu.VMEM((seq, HD), BF16),
            pltpu.VMEM((seq, qcols), BF16),
            pltpu.VMEM((seq, qcols), BF16),
            block, block, block, block, block, block, wide, wide,
            pltpu.VMEM((bits, 1, qcols), F32),
            pltpu.VMEM((bits, 1, qcols), F32),
            pltpu.VMEM((2, 1, d), F32),
            pltpu.VMEM((2, 1, d), F32),
            dma((2, kc)), dma((nc,)), dma((7,)),
            dma((kc,)), dma((kc,)), dma((kc,)), dma((kc,)), dma((kc,)), dma((kc,)),
            dma((kvcols // HD, 2)), dma((2, 2)),
            dma((nc,)), dma((nc,)), dma((nc,)), dma((nc,)), dma((nc,)), dma((nc,)),
            dma((bits,)), dma((bits,)), dma((2,)), dma((2,)),
        ],
        compiler_params=pltpu.CompilerParams(
            collective_id=0, has_side_effects=True, vmem_limit_bytes=63300000
        ),
    )(
        tokens.reshape(rows, d), gain, wq, bq, wkv, bkv, wo, check_weights, cosine, sine,
    )
    attended, checksum = pl.pallas_call(
        settle_kernel,
        out_shape=(jax.ShapeDtypeStruct((rows, d), BF16), jax.ShapeDtypeStruct((d,), F32)),
        in_specs=[vmem, vmem],
        out_specs=(vmem, vmem),
    )(attended, checksum)
    return attended.reshape(1, rows, d), checksum


def solution(mesh):
    placed = (
        P("dp", "tensor", None),
        P(),
        P(None, "tensor"),
        P("tensor"),
        P(None, "tensor"),
        P("tensor"),
        P("tensor", None),
        P("dp", None),
    )
    ndp, n_tensor = mesh.shape["dp"], mesh.shape["tensor"]

    def local(tokens, gain, wq, bq, wkv, bkv, wo, check_weights):
        whole_heads = wkv.shape[1] == 2 * HD and wq.shape[1] == HEADS // KV * HD
        if n_tensor == KV and whole_heads and ndp & (ndp - 1) == 0:
            return fused(ndp, n_tensor, tokens, gain, wq, bq, wkv, bkv, wo, check_weights)
        return general(tokens, gain, wq, bq, wkv, bkv, wo, check_weights)

    return jax.shard_map(
        local, mesh=mesh, in_specs=placed, out_specs=(P("dp", "tensor", None), P()), check_vma=False
    )
```
